32 devices in a mesh: win: 2 (over y), row: 16 (over z, x, core).
Axes of the slice: x: 2, y: 2, z: 4, core: 2. Of those that a mesh axis runs over, the one named last changes fastest.
Arguments:
- spectra: bfloat16 [32, 2, 32768], P(('win', 'row')), parts along dimension 0, may hold values from -6 to 6
- pair_mask: int32 [16, 16], P('row'), may hold values from 0 to 1, as said below
- available: int32 [32], P('win'), parts along dimension 0, may hold values 0 or 1
Outputs:
- correlations: float32 [32, 16, 8192], P(('win', 'row')), parts along dimension 0
The draws below stay inside these ranges and needn't reach their ends.
There are 2 independent parts, one for each index of `win`. The reference program is written for one: setup_inputs(seed, part) draws one part's arguments, and reference() takes and returns one part's arrays. A program takes and returns all parts, laid end to end along the dimension named above; an argument that names none is the same for every part. Nothing has to cross between parts.
Inputs may be any that keep to these rules, and one draw needn't show every extreme that they name: pair_mask[i, j] is 0 wherever j <= i.
All inputs are finite; a program needn't handle non-finite values.
Results may differ from the reference program's by a relative error of at most 0.0003.
Values may be sent and summed in bfloat16 or wider, within the bound.
A program may use at most 128 MiB of HBM per device.

```python
import math
import jax
import jax.numpy as jnp
from jax import lax

STATIONS = 16
FREQ = 32768
LAGS = 8192


def draw_pair_mask(key, part):
    picks = jax.random.randint(key, (STATIONS, STATIONS), 0, 4)
    rows = lax.broadcasted_iota(jnp.int32, (STATIONS, STATIONS), 0)
    cols = lax.broadcasted_iota(jnp.int32, (STATIONS, STATIONS), 1)
    return jnp.where((cols > rows) & (picks < 3), 1, 0).astype(jnp.int32)


def place_ends(result, key, low, largest):
    dims = result.shape
    place = [jax.random.randint(jax.random.fold_in(key, axis), (), 0, dims[axis]) for axis in range(len(dims))]
    result = result.at[tuple(place)].set(low)
    longest = dims.index(max(dims))
    place[longest] = (place[longest] + 1) % dims[longest]
    return result.at[tuple(place)].set(largest)


def level_of(own_key, extent, cuts, low, largest):
    def one(axis_at, parts):
        steps = jax.random.uniform(jax.random.fold_in(jax.random.fold_in(own_key, 6), axis_at), (parts,), jnp.float32, low / len(cuts), largest / len(cuts))
        return jnp.repeat(jnp.exp(steps), extent[axis_at] // parts).reshape((-1,) + (1,) * (len(extent) - axis_at - 1))

    gain = one(*cuts[0])
    for cut in cuts[1:]:
        gain = gain * one(*cut)
    return gain


def normal_values(key, shape, spread, bound, shards=(), held_as=jnp.bfloat16):
    values = spread * jax.random.normal(key, shape, jnp.float32)
    if shards:
        values = values * level_of(key, shape, shards, -0.22, 0.18)
    return jnp.clip(values, -bound, bound).astype(held_as)


def setup_inputs(seed: int = 0, part: int = 0) -> dict:
    streams_of = jax.random.split(jax.random.key(seed), 4)
    part_splits = jax.random.split(jax.random.fold_in(streams_of[3], part), 4)
    return {
        "spectra": normal_values(part_splits[0], (STATIONS, 2, FREQ), 1.0, 6.0, ((0, 16),)),
        "pair_mask": draw_pair_mask(jax.random.fold_in(streams_of[3], 71), part),
        "available": place_ends((jax.random.randint(part_splits[2], (STATIONS,), 0, 8) < 7).astype(jnp.int32), jax.random.fold_in(part_splits[2], 1), 0, 1),
    }


def reference(spectra, pair_mask, available):
    stations = spectra.shape[0]
    freq = spectra.shape[2]
    nfft = 2 * freq
    half = LAGS // 2
    whole = spectra.astype(jnp.float32)
    flags = available.astype(jnp.float32)
    scale = nfft / math.sqrt(8.0 * freq)

    def one_row(item):
        own, mask_row, own_flag = item
        real_part = own[0][None, :] * whole[:, 0, :] + own[1][None, :] * whole[:, 1, :]
        imag_part = own[0][None, :] * whole[:, 1, :] - own[1][None, :] * whole[:, 0, :]
        imag_part = imag_part.at[:, 0].set(0.0)
        nyquist = jnp.zeros((stations, 1), real_part.dtype)
        spectrum = lax.complex(jnp.concatenate([real_part, nyquist], axis=1), jnp.concatenate([imag_part, nyquist], axis=1))
        series = jnp.fft.irfft(spectrum, n=nfft, axis=1)
        lagged = jnp.concatenate([series[:, nfft - half:], series[:, :half]], axis=1) * scale
        return lagged * (mask_row.astype(lagged.dtype) * own_flag * flags)[:, None]
    return lax.map(one_row, (whole, pair_mask, flags))
```

```python
import functools
import math

import jax
import jax.numpy as jnp
import numpy as np
from jax import lax
from jax.experimental import pallas as pl
from jax.experimental.pallas import tpu as pltpu
from jax.sharding import PartitionSpec as P

LAGS = 8192
MESH = pl.DeviceIdType.MESH
PIECES = 2
LINE = 2
CORES = 2


def split(value):
    high = value.astype(jnp.bfloat16)
    low = (value - high.astype(jnp.float32)).astype(jnp.bfloat16)
    return high, low


def build_tables(freq, lags):
    nfft = 2 * freq
    inner = min(128, lags // 2)
    column = nfft // inner
    depth = freq // column
    outer = lags // inner
    centre = lags // 2
    turn = 2.0 * np.pi
    t_inner = np.arange(inner)[:, None]
    first = turn * ((t_inner * np.arange(depth)[None, :]) % inner) / inner
    cos_first, sin_first = np.cos(first), np.sin(first)
    one = np.block([[cos_first, -sin_first], [sin_first, cos_first]]).astype(np.float32)
    k_column = np.arange(column)[None, :]
    twist = turn * ((k_column * (t_inner - centre)) % nfft) / nfft
    second = turn * ((np.arange(outer)[:, None] * k_column) % column) / column
    two = np.concatenate([np.cos(second), -np.sin(second)], axis=1).astype(np.float32)

    def halves(table):
        high = table.astype(jnp.bfloat16)
        low = (table - high.astype(np.float32)).astype(jnp.bfloat16)
        return high, low

    one_high, one_low = halves(one)
    two_high, two_low = halves(two)
    return (
        np.concatenate([one_high, one_high, one_low], axis=1),
        np.stack([np.cos(twist), np.sin(twist)]).astype(np.float32),
        np.concatenate([two_high, two_low], axis=0),
    )


def kernel(
    devices,
    mask_ref,
    avail_ref,
    x_ref,
    one_ref,
    twist_ref,
    two_ref,
    out_ref,
    buf,
    own,
    res,
    recv,
    send_z,
    send_x,
    send_d,
):
    planes = devices // (LINE * CORES)
    me = lax.axis_index("row")
    core = me % CORES
    chip = me // CORES
    side = chip % LINE
    plane = chip // LINE
    depth = x_ref.shape[1]
    inner = twist_ref.shape[1]
    outer = two_ref.shape[0] // 2
    freq = depth * x_ref.shape[2]
    scale = 2.0 / math.sqrt(8.0 * freq)
    rows = depth // PIECES

    def index(p, s, c):
        return (p * LINE + s) * CORES + c

    below = index(plane - 1, side, core)
    above = index(plane + 1, side, core)
    beside = index(plane, 1 - side, core)
    twin = index(plane, side, 1 - core)

    def greet(device):
        pl.semaphore_signal(barrier, inc=1, device_id={"row": device}, device_id_type=MESH)

    def piece(ref, k):
        return ref.at[:, pl.ds(k * rows, rows), :]

    def copy(station, p, k, sem, kind, device, mine=False):
        slot = piece(buf.at[station], k)
        return pltpu.make_async_remote_copy(
            src_ref=piece(x_ref, k) if mine else slot,
            dst_ref=slot,
            send_sem=sem,
            recv_sem=recv.at[kind, p, k],
            device_id={"row": device},
            device_id_type=MESH,
        )

    def down(p, k, mine=False):
        return copy(index(p, side, core), p, k, send_z.at[p, k], 0, below, mine)

    def across(p, k, mine=False):
        return copy(index(p, side, core), p, k, send_x.at[p, k], 1, beside, mine)

    def over(p, k, mine=False):
        return copy(index(p, side, core), p, k, send_d.at[0, p, k], 2, twin, mine)

    def over_side(p, k):
        return copy(index(p, 1 - side, core), p, k, send_d.at[1, p, k], 3, twin)

    def arrived(station, p, k, kind):
        slot = piece(buf.at[station], k)
        pltpu.make_async_remote_copy(
            src_ref=slot,
            dst_ref=slot,
            send_sem=send_z.at[p, k],
            recv_sem=recv.at[kind, p, k],
            device_id={"row": twin},
            device_id_type=MESH,
        ).wait_recv()

    barrier = pltpu.get_barrier_semaphore()
    greet(beside)
    greet(twin)

    @pl.when(plane > 0)
    def _():
        greet(below)

    @pl.when(plane < planes - 1)
    def _():
        greet(above)

    first = (
        (lax.broadcasted_iota(jnp.int32, (depth, x_ref.shape[2]), 0) == 0)
        & (lax.broadcasted_iota(jnp.int32, (depth, x_ref.shape[2]), 1) == 0)
    )
    weight = jnp.where(first, 0.5, 1.0)
    own[0] = x_ref[0].astype(jnp.float32) * weight
    own[1] = x_ref[1].astype(jnp.float32) * weight

    peers = 2 + jnp.where(plane > 0, 1, 0) + jnp.where(plane < planes - 1, 1, 0)
    pl.semaphore_wait(barrier, peers)

    for k in range(PIECES):

        @pl.when(plane > 0)
        def _():
            down(plane, k, True).start()

        @pl.when(side == 1)
        def _():
            across(plane, k, True).start()

        @pl.when(core == 1)
        def _():
            over(plane, k, True).start()

    def clear(g, carry):
        res[g] = jnp.zeros(res.shape[1:], jnp.float32)
        return carry

    lax.fori_loop(0, devices, clear, 0)

    def correlate(station):
        own_re, own_im = own[0], own[1]
        re = buf[station, 0].astype(jnp.float32)
        im = buf[station, 1].astype(jnp.float32)
        re_high, re_low = split(own_re * re + own_im * im)
        im_high, im_low = split(own_re * im - own_im * re)
        cross = jnp.concatenate([re_high, im_high, re_low, im_low, re_high, im_high], axis=0)
        mixed = jnp.dot(one_ref[...], cross, preferred_element_type=jnp.float32)
        real, imag = mixed[:inner], mixed[inner:]
        turned_re = real * twist_ref[0] - imag * twist_ref[1]
        turned_im = real * twist_ref[1] + imag * twist_ref[0]
        high, low = split(jnp.concatenate([turned_re, turned_im], axis=1))
        both = jnp.concatenate([high, low], axis=0)
        summed = lax.dot_general(
            two_ref[...],
            both,
            (((1,), (1,)), ((), ())),
            preferred_element_type=jnp.float32,
        )
        total = (summed[:outer, :inner] + summed[:outer, inner:]) + (
            summed[outer:, :inner] + summed[outer:, inner:]
        )
        flag = (mask_ref[0, station] * avail_ref[me] * avail_ref[station]).astype(jnp.float32)
        res[station] = total * (flag * scale)

    def side_in(p):
        for k in range(PIECES):
            arrived(index(p, 1 - side, core), p, k, 1)
            over_side(p, k).start()

    @pl.when(side == 0)
    def _():
        side_in(plane)

    @pl.when(core == 0)
    def _():
        for k in range(PIECES):
            arrived(twin, plane, k, 2)
        correlate(twin)

    @pl.when(side == 0)
    def _():
        correlate(beside)
        for k in range(PIECES):
            arrived(index(plane, 1 - side, 1 - core), plane, k, 3)
        correlate(index(plane, 1 - side, 1 - core))

    def step(p, carry):
        for k in range(PIECES):
            arrived(index(p, side, core), p, k, 0)

            @pl.when(plane > 0)
            def _():
                down(p, k).start()

            across(p, k).start()
            over(p, k).start()
        correlate(index(p, side, core))
        side_in(p)
        for k in range(PIECES):
            arrived(index(p, side, 1 - core), p, k, 2)
        correlate(index(p, side, 1 - core))
        correlate(index(p, 1 - side, core))
        for k in range(PIECES):
            arrived(index(p, 1 - side, 1 - core), p, k, 3)
        correlate(index(p, 1 - side, 1 - core))
        return carry

    lax.fori_loop(plane + 1, planes, step, 0)

    group = math.gcd(devices, 8)

    def place(g, carry):
        at = pl.multiple_of(g * group, group)
        for o in range(outer):
            out_ref[pl.ds(at, group), o * inner : (o + 1) * inner] = res[pl.ds(at, group), o, :]
        return carry

    lax.fori_loop(0, devices // group, place, 0)

    for k in range(PIECES):

        @pl.when(plane > 0)
        def _():
            down(plane, k, True).wait_send()

        @pl.when(side == 1)
        def _():
            across(plane, k, True).wait_send()

        @pl.when(side == 0)
        def _():
            over_side(plane, k).wait_send()

        @pl.when(core == 1)
        def _():
            over(plane, k, True).wait_send()

    def finish(p, carry):
        for k in range(PIECES):

            @pl.when(plane > 0)
            def _():
                down(p, k).wait_send()

            across(p, k).wait_send()
            over(p, k).wait_send()
            over_side(p, k).wait_send()
        return carry

    lax.fori_loop(plane + 1, planes, finish, 0)


def per_device(spectra, pair_mask, available):
    devices = lax.axis_size("row")
    freq = spectra.shape[2]
    one, twist, two = build_tables(freq, LAGS)
    inner, column = twist.shape[1:]
    depth = freq // column
    planes = devices // (LINE * CORES)
    vmem = pl.BlockSpec(memory_space=pltpu.VMEM)
    smem = pl.BlockSpec(memory_space=pltpu.SMEM)
    rows = pl.pallas_call(
        functools.partial(kernel, devices),
        out_shape=jax.ShapeDtypeStruct((devices, LAGS), jnp.float32),
        in_specs=[smem, smem, vmem, vmem, vmem, vmem],
        out_specs=vmem,
        scratch_shapes=[
            pltpu.VMEM((devices, 2, depth, column), jnp.bfloat16),
            pltpu.VMEM((2, depth, column), jnp.float32),
            pltpu.VMEM((devices, LAGS // inner, inner), jnp.float32),
            pltpu.SemaphoreType.DMA((4, planes, PIECES)),
            pltpu.SemaphoreType.DMA((planes, PIECES)),
            pltpu.SemaphoreType.DMA((planes, PIECES)),
            pltpu.SemaphoreType.DMA((2, planes, PIECES)),
        ],
        compiler_params=pltpu.CompilerParams(
            collective_id=0, has_side_effects=True, vmem_limit_bytes=48 * 1024 * 1024
        ),
    )(
        pair_mask,
        available,
        spectra.reshape(2, depth, column),
        jnp.asarray(one),
        jnp.asarray(twist),
        jnp.asarray(two),
    )
    return rows[None]


def solution(mesh):
    return jax.shard_map(
        per_device,
        mesh=mesh,
        in_specs=(P(("win", "row"), None, None), P("row", None), P("win")),
        out_specs=P(("win", "row"), None, None),
        check_vma=False,
    )
```

```python
import functools
import math

import jax
import jax.numpy as jnp
import numpy as np
from jax import lax
from jax.experimental import pallas as pl
from jax.experimental.pallas import tpu as pltpu
from jax.sharding import PartitionSpec as P

LAGS = 8192
MESH = pl.DeviceIdType.MESH
PIECES = 2
DETOUR = 1
LINE = 2
CORES = 2


def split(value):
    high = value.astype(jnp.bfloat16)
    low = (value - high.astype(jnp.float32)).astype(jnp.bfloat16)
    return high, low


def build_tables(freq, lags):
    nfft = 2 * freq
    inner = min(128, lags // 2)
    column = nfft // inner
    depth = freq // column
    outer = lags // inner
    centre = lags // 2
    turn = 2.0 * np.pi
    t_inner = np.arange(inner)[:, None]
    first = turn * ((t_inner * np.arange(depth)[None, :]) % inner) / inner
    cos_first, sin_first = np.cos(first), np.sin(first)
    one = np.block([[cos_first, -sin_first], [sin_first, cos_first]]).astype(np.float32)
    k_column = np.arange(column)[None, :]
    twist = turn * ((k_column * (t_inner - centre)) % nfft) / nfft
    second = turn * ((np.arange(outer)[:, None] * k_column) % column) / column
    two = np.concatenate([np.cos(second), -np.sin(second)], axis=1).astype(np.float32)

    def halves(table):
        high = table.astype(jnp.bfloat16)
        low = (table - high.astype(np.float32)).astype(jnp.bfloat16)
        return high, low

    one_high, one_low = halves(one)
    two_high, two_low = halves(two)
    return (
        np.concatenate([one_high, one_high, one_low], axis=1),
        np.stack([np.cos(twist), np.sin(twist)]).astype(np.float32),
        np.concatenate([two_high, two_low], axis=0),
    )


def kernel(
    devices,
    mask_ref,
    avail_ref,
    x_ref,
    one_hbm,
    twist_hbm,
    two_hbm,
    out_ref,
    one_ref,
    twist_ref,
    two_ref,
    table_sem,
    buf,
    own,
    res,
    recv,
    send_z,
    send_x,
    send_d,
):
    planes = devices // (LINE * CORES)
    me = lax.axis_index("row")
    core = me % CORES
    chip = me // CORES
    side = chip % LINE
    plane = chip // LINE
    depth = x_ref.shape[1]
    inner = twist_ref.shape[1]
    outer = two_ref.shape[0] // 2
    freq = depth * x_ref.shape[2]
    scale = 2.0 / math.sqrt(8.0 * freq)
    rows = depth // PIECES

    def index(p, s, c):
        return (p * LINE + s) * CORES + c

    below = index(plane - 1, side, core)
    above = index(plane + 1, side, core)
    beside = index(plane, 1 - side, core)
    twin = index(plane, side, 1 - core)

    def greet(device):
        pl.semaphore_signal(barrier, inc=1, device_id={"row": device}, device_id_type=MESH)

    def piece(ref, k):
        return ref.at[:, pl.ds(k * rows, rows), :]

    def copy(station, p, k, sem, kind, device, mine=False):
        slot = piece(buf.at[station], k)
        return pltpu.make_async_remote_copy(
            src_ref=piece(x_ref, k) if mine else slot,
            dst_ref=slot,
            send_sem=sem,
            recv_sem=recv.at[kind, p, k],
            device_id={"row": device},
            device_id_type=MESH,
        )

    def down(p, k, mine=False):
        return copy(index(p, side, core), p, k, send_z.at[p, k], 0, below, mine)

    def across(p, k, mine=False):
        return copy(index(p, side, core), p, k, send_x.at[p, k], 1, beside, mine)

    def over(p, k, mine=False):
        return copy(index(p, side, core), p, k, send_d.at[0, p, k], 2, twin, mine)

    def down_side(k):
        return copy(index(plane, 1 - side, core), plane, k, send_x.at[plane, k], 1, below)

    def over_side(p, k):
        return copy(index(p, 1 - side, core), p, k, send_d.at[1, p, k], 3, twin)

    def arrived(station, p, k, kind):
        slot = piece(buf.at[station], k)
        pltpu.make_async_remote_copy(
            src_ref=slot,
            dst_ref=slot,
            send_sem=send_z.at[p, k],
            recv_sem=recv.at[kind, p, k],
            device_id={"row": twin},
            device_id_type=MESH,
        ).wait_recv()

    loads = [
        pltpu.make_async_copy(source, target, table_sem.at[n])
        for n, (source, target) in enumerate(
            ((one_hbm, one_ref), (twist_hbm, twist_ref), (two_hbm, two_ref))
        )
    ]
    barrier = pltpu.get_barrier_semaphore()
    greet(beside)
    greet(twin)

    @pl.when(plane > 0)
    def _():
        greet(below)

    @pl.when(plane < planes - 1)
    def _():
        greet(above)

    for load in loads:
        load.start()

    peers = 2 + jnp.where(plane > 0, 1, 0) + jnp.where(plane < planes - 1, 1, 0)
    pl.semaphore_wait(barrier, peers)

    for k in range(PIECES):

        @pl.when(plane > 0)
        def _():
            down(plane, k, True).start()

        @pl.when(side == 1)
        def _():
            across(plane, k, True).start()

        @pl.when(core == 1)
        def _():
            over(plane, k, True).start()

    first = (
        (lax.broadcasted_iota(jnp.int32, (depth, x_ref.shape[2]), 0) == 0)
        & (lax.broadcasted_iota(jnp.int32, (depth, x_ref.shape[2]), 1) == 0)
    )
    weight = jnp.where(first, 0.5, 1.0)
    own[0] = x_ref[0].astype(jnp.float32) * weight
    own[1] = x_ref[1].astype(jnp.float32) * weight

    def clear(g, carry):
        res[g] = jnp.zeros(res.shape[1:], jnp.float32)
        return carry

    lax.fori_loop(0, devices, clear, 0)

    def correlate(station):
        own_re, own_im = own[0], own[1]
        re = buf[station, 0].astype(jnp.float32)
        im = buf[station, 1].astype(jnp.float32)
        re_high, re_low = split(own_re * re + own_im * im)
        im_high, im_low = split(own_re * im - own_im * re)
        cross = jnp.concatenate([re_high, im_high, re_low, im_low, re_high, im_high], axis=0)
        mixed = jnp.dot(one_ref[...], cross, preferred_element_type=jnp.float32)
        real, imag = mixed[:inner], mixed[inner:]
        turned_re = real * twist_ref[0] - imag * twist_ref[1]
        turned_im = real * twist_ref[1] + imag * twist_ref[0]
        high, low = split(jnp.concatenate([turned_re, turned_im], axis=1))
        both = jnp.concatenate([high, low], axis=0)
        summed = lax.dot_general(
            two_ref[...],
            both,
            (((1,), (1,)), ((), ())),
            preferred_element_type=jnp.float32,
        )
        total = (summed[:outer, :inner] + summed[:outer, inner:]) + (
            summed[outer:, :inner] + summed[outer:, inner:]
        )
        flag = (mask_ref[0, station] * avail_ref[me] * avail_ref[station]).astype(jnp.float32)
        res[station] = total * (flag * scale)

    def column_in(p):
        for k in range(PIECES):
            arrived(index(p, side, core), p, k, 0)

            @pl.when(plane > 0)
            def _():
                down(p, k).start()

            if k < DETOUR:

                @pl.when((side == 0) | (p > plane + 1))
                def _():
                    across(p, k).start()

            else:
                across(p, k).start()
            over(p, k).start()

    def side_in(p):
        for k in range(PIECES):
            arrived(index(p, 1 - side, core), p, k, 1)
            over_side(p, k).start()
            if k < DETOUR:

                @pl.when((p == plane) & (plane > 0))
                def _():
                    down_side(k).start()

    def twin_column(p):
        for k in range(PIECES):
            arrived(index(p, side, 1 - core), p, k, 2)
        correlate(index(p, side, 1 - core))

    def twin_side(p):
        correlate(index(p, 1 - side, core))
        for k in range(PIECES):
            arrived(index(p, 1 - side, 1 - core), p, k, 3)
        correlate(index(p, 1 - side, 1 - core))

    for load in loads:
        load.wait()

    @pl.when(core == 0)
    def _():
        twin_column(plane)

    def step(p, carry):
        column_in(p)
        correlate(index(p, side, core))

        @pl.when((side == 0) | (p > plane + 1))
        def _():
            side_in(p - 1)

        twin_column(p)

        @pl.when((side == 0) | (p > plane + 1))
        def _():
            twin_side(p - 1)

        return carry

    lax.fori_loop(plane + 1, planes, step, 0)

    @pl.when((side == 0) | (plane < planes - 1))
    def _():
        side_in(planes - 1)
        twin_side(planes - 1)

    group = math.gcd(devices, 8)

    def place(g, carry):
        at = pl.multiple_of(g * group, group)
        for o in range(outer):
            out_ref[pl.ds(at, group), o * inner : (o + 1) * inner] = res[pl.ds(at, group), o, :]
        return carry

    lax.fori_loop(0, devices // group, place, 0)

    for k in range(PIECES):

        @pl.when(plane > 0)
        def _():
            down(plane, k, True).wait_send()

        @pl.when(side == 1)
        def _():
            across(plane, k, True).wait_send()

        @pl.when(side == 0)
        def _():
            over_side(plane, k).wait_send()

        if k < DETOUR:

            @pl.when((side == 0) & (plane > 0))
            def _():
                down_side(k).wait_send()

        @pl.when(core == 1)
        def _():
            over(plane, k, True).wait_send()

    def finish(p, carry):
        for k in range(PIECES):

            @pl.when(plane > 0)
            def _():
                down(p, k).wait_send()

            if k < DETOUR:

                @pl.when((side == 0) | (p > plane + 1))
                def _():
                    across(p, k).wait_send()

            else:
                across(p, k).wait_send()
            over(p, k).wait_send()
            over_side(p, k).wait_send()
        return carry

    lax.fori_loop(plane + 1, planes, finish, 0)


def per_device(spectra, pair_mask, available):
    devices = lax.axis_size("row")
    freq = spectra.shape[2]
    one, twist, two = build_tables(freq, LAGS)
    inner, column = twist.shape[1:]
    depth = freq // column
    planes = devices // (LINE * CORES)
    vmem = pl.BlockSpec(memory_space=pltpu.VMEM)
    hbm = pl.BlockSpec(memory_space=pltpu.HBM)
    smem = pl.BlockSpec(memory_space=pltpu.SMEM)
    rows = pl.pallas_call(
        functools.partial(kernel, devices),
        out_shape=jax.ShapeDtypeStruct((devices, LAGS), jnp.float32),
        in_specs=[smem, smem, vmem, hbm, hbm, hbm],
        out_specs=vmem,
        scratch_shapes=[
            pltpu.VMEM(one.shape, jnp.bfloat16),
            pltpu.VMEM(twist.shape, jnp.float32),
            pltpu.VMEM(two.shape, jnp.bfloat16),
            pltpu.SemaphoreType.DMA((3,)),
            pltpu.VMEM((devices, 2, depth, column), jnp.bfloat16),
            pltpu.VMEM((2, depth, column), jnp.float32),
            pltpu.VMEM((devices, LAGS // inner, inner), jnp.float32),
            pltpu.SemaphoreType.DMA((4, planes, PIECES)),
            pltpu.SemaphoreType.DMA((planes, PIECES)),
            pltpu.SemaphoreType.DMA((planes, PIECES)),
            pltpu.SemaphoreType.DMA((2, planes, PIECES)),
        ],
        compiler_params=pltpu.CompilerParams(
            collective_id=0, has_side_effects=True, vmem_limit_bytes=48 * 1024 * 1024
        ),
    )(
        pair_mask,
        available,
        spectra.reshape(2, depth, column),
        jnp.asarray(one),
        jnp.asarray(twist),
        jnp.asarray(two),
    )
    return rows[None]


def solution(mesh):
    return jax.shard_map(
        per_device,
        mesh=mesh,
        in_specs=(P(("win", "row"), None, None), P("row", None), P("win")),
        out_specs=P(("win", "row"), None, None),
        check_vma=False,
    )
```

```python
import functools
import math

import jax
import jax.numpy as jnp
import numpy as np
from jax import lax
from jax.experimental import pallas as pl
from jax.experimental.pallas import tpu as pltpu
from jax.sharding import PartitionSpec as P

LAGS = 8192
MESH = pl.DeviceIdType.MESH
PIECES = 2
DETOUR = 1
LINE = 2
CORES = 2
GRANT = 67_043_328


def split(value):
    high = value.astype(jnp.bfloat16)
    low = (value - high.astype(jnp.float32)).astype(jnp.bfloat16)
    return high, low


def build_tables(freq, lags):
    nfft = 2 * freq
    inner = min(128, lags // 2)
    column = nfft // inner
    depth = freq // column
    outer = lags // inner
    centre = lags // 2
    turn = 2.0 * np.pi
    t_inner = np.arange(inner)[:, None]
    first = turn * ((t_inner * np.arange(depth)[None, :]) % inner) / inner
    cos_first, sin_first = np.cos(first), np.sin(first)
    one = np.block([[cos_first, -sin_first], [sin_first, cos_first]]).astype(np.float32)
    k_column = np.arange(column)[None, :]
    twist = turn * ((k_column * (t_inner - centre)) % nfft) / nfft
    second = turn * ((np.arange(outer)[:, None] * k_column) % column) / column
    two = np.concatenate([np.cos(second), -np.sin(second)], axis=1).astype(np.float32)

    def halves(table):
        high = table.astype(jnp.bfloat16)
        low = (table - high.astype(np.float32)).astype(jnp.bfloat16)
        return high, low

    one_high, one_low = halves(one)
    two_high, two_low = halves(two)
    return (
        np.concatenate([one_high, one_high, one_low], axis=1),
        np.stack([np.cos(twist), np.sin(twist)]).astype(np.float32),
        np.concatenate([two_high, two_low], axis=0),
    )


def kernel(
    devices,
    mask_ref,
    avail_ref,
    x_ref,
    one_hbm,
    twist_hbm,
    two_hbm,
    out_ref,
    one_ref,
    twist_ref,
    two_ref,
    table_sem,
    buf,
    own,
    res,
    recv,
    send_z,
    send_x,
    send_d,
):
    planes = devices // (LINE * CORES)
    me = lax.axis_index("row")
    core = me % CORES
    chip = me // CORES
    side = chip % LINE
    plane = chip // LINE
    depth = x_ref.shape[1]
    inner = twist_ref.shape[1]
    outer = two_ref.shape[0] // 2
    freq = depth * x_ref.shape[2]
    scale = 2.0 / math.sqrt(8.0 * freq)
    rows = depth // PIECES

    def index(p, s, c):
        return (p * LINE + s) * CORES + c

    below = index(plane - 1, side, core)
    above = index(plane + 1, side, core)
    beside = index(plane, 1 - side, core)
    twin = index(plane, side, 1 - core)

    def greet(device):
        pl.semaphore_signal(barrier, inc=1, device_id={"row": device}, device_id_type=MESH)

    def piece(ref, k):
        return ref.at[:, pl.ds(k * rows, rows), :]

    def copy(station, p, k, sem, kind, device, mine=False):
        slot = piece(buf.at[station], k)
        return pltpu.make_async_remote_copy(
            src_ref=piece(x_ref, k) if mine else slot,
            dst_ref=slot,
            send_sem=sem,
            recv_sem=recv.at[kind, p, k],
            device_id={"row": device},
            device_id_type=MESH,
        )

    def down(p, k, mine=False):
        return copy(index(p, side, core), p, k, send_z.at[p, k], 0, below, mine)

    def across(p, k, mine=False):
        return copy(index(p, side, core), p, k, send_x.at[p, k], 1, beside, mine)

    def over(p, k, mine=False):
        return copy(index(p, side, core), p, k, send_d.at[0, p, k], 2, twin, mine)

    def down_side(k):
        return copy(index(plane, 1 - side, core), plane, k, send_x.at[plane, k], 1, below)

    def over_side(p, k):
        return copy(index(p, 1 - side, core), p, k, send_d.at[1, p, k], 3, twin)

    def arrived(station, p, k, kind):
        slot = piece(buf.at[station], k)
        pltpu.make_async_remote_copy(
            src_ref=slot,
            dst_ref=slot,
            send_sem=send_z.at[p, k],
            recv_sem=recv.at[kind, p, k],
            device_id={"row": twin},
            device_id_type=MESH,
        ).wait_recv()

    loads = [
        pltpu.make_async_copy(source, target, table_sem.at[n])
        for n, (source, target) in enumerate(
            ((one_hbm, one_ref), (twist_hbm, twist_ref), (two_hbm, two_ref))
        )
    ]
    barrier = pltpu.get_barrier_semaphore()
    greet(beside)
    greet(twin)

    @pl.when(plane > 0)
    def _():
        greet(below)

    @pl.when(plane < planes - 1)
    def _():
        greet(above)

    for load in loads:
        load.start()

    peers = 2 + jnp.where(plane > 0, 1, 0) + jnp.where(plane < planes - 1, 1, 0)
    pl.semaphore_wait(barrier, peers)

    for k in range(PIECES):

        @pl.when(plane > 0)
        def _():
            down(plane, k, True).start()

        @pl.when(side == 1)
        def _():
            across(plane, k, True).start()

        @pl.when(core == 1)
        def _():
            over(plane, k, True).start()

    first = (
        (lax.broadcasted_iota(jnp.int32, (depth, x_ref.shape[2]), 0) == 0)
        & (lax.broadcasted_iota(jnp.int32, (depth, x_ref.shape[2]), 1) == 0)
    )
    weight = jnp.where(first, 0.5, 1.0)
    own[0] = x_ref[0].astype(jnp.float32) * weight
    own[1] = x_ref[1].astype(jnp.float32) * weight

    def clear(g, carry):
        res[g] = jnp.zeros(res.shape[1:], jnp.float32)
        return carry

    lax.fori_loop(0, devices, clear, 0)

    def correlate(station):
        own_re, own_im = own[0], own[1]
        re = buf[station, 0].astype(jnp.float32)
        im = buf[station, 1].astype(jnp.float32)
        re_high, re_low = split(own_re * re + own_im * im)
        im_high, im_low = split(own_re * im - own_im * re)
        cross = jnp.concatenate([re_high, im_high, re_low, im_low, re_high, im_high], axis=0)
        mixed = jnp.dot(one_ref[...], cross, preferred_element_type=jnp.float32)
        real, imag = mixed[:inner], mixed[inner:]
        turned_re = real * twist_ref[0] - imag * twist_ref[1]
        turned_im = real * twist_ref[1] + imag * twist_ref[0]
        high, low = split(jnp.concatenate([turned_re, turned_im], axis=1))
        both = jnp.concatenate([high, low], axis=0)
        summed = lax.dot_general(
            two_ref[...],
            both,
            (((1,), (1,)), ((), ())),
            preferred_element_type=jnp.float32,
        )
        total = (summed[:outer, :inner] + summed[:outer, inner:]) + (
            summed[outer:, :inner] + summed[outer:, inner:]
        )
        flag = (mask_ref[0, station] * avail_ref[me] * avail_ref[station]).astype(jnp.float32)
        res[station] = total * (flag * scale)

    def column_in(p):
        for k in range(PIECES):
            arrived(index(p, side, core), p, k, 0)

            @pl.when(plane > 0)
            def _():
                down(p, k).start()

            if k < DETOUR:

                @pl.when((side == 0) | (p > plane + 1))
                def _():
                    across(p, k).start()

            else:
                across(p, k).start()
            over(p, k).start()

    def side_in(p):
        for k in range(PIECES):
            arrived(index(p, 1 - side, core), p, k, 1)
            over_side(p, k).start()
            if k < DETOUR:

                @pl.when((p == plane) & (plane > 0))
                def _():
                    down_side(k).start()

    def twin_column(p):
        for k in range(PIECES):
            arrived(index(p, side, 1 - core), p, k, 2)
        correlate(index(p, side, 1 - core))

    def twin_side(p):
        correlate(index(p, 1 - side, core))
        for k in range(PIECES):
            arrived(index(p, 1 - side, 1 - core), p, k, 3)
        correlate(index(p, 1 - side, 1 - core))

    for load in loads:
        load.wait()

    @pl.when(core == 0)
    def _():
        twin_column(plane)

    def step(p, carry):
        column_in(p)
        correlate(index(p, side, core))

        @pl.when((side == 0) | (p > plane + 1))
        def _():
            side_in(p - 1)

        twin_column(p)

        @pl.when((side == 0) | (p > plane + 1))
        def _():
            twin_side(p - 1)

        return carry

    lax.fori_loop(plane + 1, planes, step, 0)

    @pl.when((side == 0) | (plane < planes - 1))
    def _():
        side_in(planes - 1)
        twin_side(planes - 1)

    group = math.gcd(devices, 8)

    def place(g, carry):
        at = pl.multiple_of(g * group, group)
        for o in range(outer):
            out_ref[pl.ds(at, group), o * inner : (o + 1) * inner] = res[pl.ds(at, group), o, :]
        return carry

    lax.fori_loop(0, devices // group, place, 0)

    for k in range(PIECES):

        @pl.when(plane > 0)
        def _():
            down(plane, k, True).wait_send()

        @pl.when(side == 1)
        def _():
            across(plane, k, True).wait_send()

        @pl.when(side == 0)
        def _():
            over_side(plane, k).wait_send()

        if k < DETOUR:

            @pl.when((side == 0) & (plane > 0))
            def _():
                down_side(k).wait_send()

        @pl.when(core == 1)
        def _():
            over(plane, k, True).wait_send()

    def finish(p, carry):
        for k in range(PIECES):

            @pl.when(plane > 0)
            def _():
                down(p, k).wait_send()

            if k < DETOUR:

                @pl.when((side == 0) | (p > plane + 1))
                def _():
                    across(p, k).wait_send()

            else:
                across(p, k).wait_send()
            over(p, k).wait_send()
            over_side(p, k).wait_send()
        return carry

    lax.fori_loop(plane + 1, planes, finish, 0)


def per_device(spectra, pair_mask, available):
    devices = lax.axis_size("row")
    freq = spectra.shape[2]
    one, twist, two = build_tables(freq, LAGS)
    inner, column = twist.shape[1:]
    depth = freq // column
    planes = devices // (LINE * CORES)
    vmem = pl.BlockSpec(memory_space=pltpu.VMEM)
    hbm = pl.BlockSpec(memory_space=pltpu.HBM)
    smem = pl.BlockSpec(memory_space=pltpu.SMEM)
    rows = pl.pallas_call(
        functools.partial(kernel, devices),
        out_shape=jax.ShapeDtypeStruct((devices, LAGS), jnp.float32),
        in_specs=[smem, smem, vmem, hbm, hbm, hbm],
        out_specs=vmem,
        scratch_shapes=[
            pltpu.VMEM(one.shape, jnp.bfloat16),
            pltpu.VMEM(twist.shape, jnp.float32),
            pltpu.VMEM(two.shape, jnp.bfloat16),
            pltpu.SemaphoreType.DMA((3,)),
            pltpu.VMEM((devices, 2, depth, column), jnp.bfloat16),
            pltpu.VMEM((2, depth, column), jnp.float32),
            pltpu.VMEM((devices, LAGS // inner, inner), jnp.float32),
            pltpu.SemaphoreType.DMA((4, planes, PIECES)),
            pltpu.SemaphoreType.DMA((planes, PIECES)),
            pltpu.SemaphoreType.DMA((planes, PIECES)),
            pltpu.SemaphoreType.DMA((2, planes, PIECES)),
        ],
        compiler_params=pltpu.CompilerParams(
            collective_id=0, has_side_effects=True, vmem_limit_bytes=GRANT
        ),
    )(
        pair_mask,
        available,
        spectra.reshape(2, depth, column),
        jnp.asarray(one),
        jnp.asarray(twist),
        jnp.asarray(two),
    )
    return rows[None]


def solution(mesh):
    return jax.shard_map(
        per_device,
        mesh=mesh,
        in_specs=(P(("win", "row"), None, None), P("row", None), P("win")),
        out_specs=P(("win", "row"), None, None),
        check_vma=False,
    )
```

```python
import functools
import math

import jax
import jax.numpy as jnp
import numpy as np
from jax import lax
from jax.experimental import pallas as pl
from jax.experimental.pallas import tpu as pltpu
from jax.sharding import PartitionSpec as P

LAGS = 8192
MESH = pl.DeviceIdType.MESH
PIECES = 4
DETOUR = 2
LINE = 2
CORES = 2
LANES = 128


def split(value):
    high = value.astype(jnp.bfloat16)
    low = (value - high.astype(jnp.float32)).astype(jnp.bfloat16)
    return high, low


def build_tables(freq, lags):
    nfft = 2 * freq
    inner = min(128, lags // 2)
    column = nfft // inner
    depth = freq // column
    outer = lags // inner
    centre = lags // 2
    turn = 2.0 * np.pi
    t_inner = np.arange(inner)[:, None]
    first = turn * ((t_inner * np.arange(depth)[None, :]) % inner) / inner
    cos_first, sin_first = np.cos(first), np.sin(first)
    one = np.block([[cos_first, -sin_first], [sin_first, cos_first]]).astype(np.float32)
    k_column = np.arange(column)[None, :]
    twist = turn * ((k_column * (t_inner - centre)) % nfft) / nfft
    second = turn * ((np.arange(outer)[:, None] * k_column) % column) / column
    two = np.concatenate([np.cos(second), -np.sin(second)], axis=1).astype(np.float32)

    def stacked(table):
        return np.concatenate(np.split(table, table.shape[1] // LANES, axis=1), axis=0)

    turns = [np.cos(twist).astype(np.float32), np.sin(twist).astype(np.float32)]
    packed = np.concatenate([stacked(part) for part in (*turns, one, two)], axis=0)
    return packed, inner, column, outer


def kernel(
    devices,
    mask_ref,
    avail_ref,
    x_ref,
    packed_ref,
    out_ref,
    one_ref,
    twist_ref,
    two_ref,
    buf,
    own,
    res,
    recv,
    send_z,
    send_x,
    send_d,
):
    planes = devices // (LINE * CORES)
    me = lax.axis_index("row")
    core = me % CORES
    chip = me // CORES
    side = chip % LINE
    plane = chip // LINE
    depth, column = x_ref.shape[1:]
    rows = depth // PIECES
    inner = twist_ref.shape[1]
    outer = two_ref.shape[0] // 2
    scale = 2.0 / math.sqrt(8.0 * depth * column)

    def index(p, s, c):
        return (p * LINE + s) * CORES + c

    below = index(plane - 1, side, core)
    above = index(plane + 1, side, core)
    beside = index(plane, 1 - side, core)
    twin = index(plane, side, 1 - core)

    def greet(device):
        pl.semaphore_signal(barrier, inc=1, device_id={"row": device}, device_id_type=MESH)

    def copy(station, p, k, sem, kind, device, mine=False):
        slot = buf.at[station, k]
        return pltpu.make_async_remote_copy(
            src_ref=x_ref.at[:, pl.ds(k * rows, rows), :] if mine else slot,
            dst_ref=slot,
            send_sem=sem,
            recv_sem=recv.at[kind, p, k],
            device_id={"row": device},
            device_id_type=MESH,
        )

    def down(p, k, mine=False):
        return copy(index(p, side, core), p, k, send_z.at[p, k], 0, below, mine)

    def across(p, k, mine=False):
        return copy(index(p, side, core), p, k, send_x.at[p, k], 1, beside, mine)

    def over(p, k, mine=False):
        return copy(index(p, side, core), p, k, send_d.at[0, p, k], 2, twin, mine)

    def down_side(k):
        return copy(index(plane, 1 - side, core), plane, k, send_x.at[plane, k], 1, below)

    def over_side(p, k):
        return copy(index(p, 1 - side, core), p, k, send_d.at[1, p, k], 3, twin)

    def arrived(station, p, k, kind):
        slot = buf.at[station, k]
        pltpu.make_async_remote_copy(
            src_ref=slot,
            dst_ref=slot,
            send_sem=send_z.at[p, k],
            recv_sem=recv.at[kind, p, k],
            device_id={"row": twin},
            device_id_type=MESH,
        ).wait_recv()

    barrier = pltpu.get_barrier_semaphore()
    greet(beside)
    greet(twin)

    @pl.when(plane > 0)
    def _():
        greet(below)

    @pl.when(plane < planes - 1)
    def _():
        greet(above)

    peers = 2 + jnp.where(plane > 0, 1, 0) + jnp.where(plane < planes - 1, 1, 0)
    pl.semaphore_wait(barrier, peers)

    for k in range(PIECES):

        @pl.when(plane > 0)
        def _():
            down(plane, k, True).start()

        @pl.when(side == 1)
        def _():
            across(plane, k, True).start()

        @pl.when(core == 1)
        def _():
            over(plane, k, True).start()

    first = (
        (lax.broadcasted_iota(jnp.int32, (depth, column), 0) == 0)
        & (lax.broadcasted_iota(jnp.int32, (depth, column), 1) == 0)
    )
    weight = jnp.where(first, 0.5, 1.0)
    own[0] = x_ref[0].astype(jnp.float32) * weight
    own[1] = x_ref[1].astype(jnp.float32) * weight

    at = 0
    for part in range(2):
        for b in range(column // LANES):
            twist_ref[part, :, b * LANES : (b + 1) * LANES] = packed_ref[at : at + inner, :]
            at += inner
    for b in range(2 * depth // LANES):
        high, low = split(packed_ref[at : at + 2 * inner, :])
        for n, term in enumerate((high, high, low)):
            left = 2 * depth * n + b * LANES
            one_ref[:, left : left + LANES] = term
        at += 2 * inner
    for b in range(2 * column // LANES):
        high, low = split(packed_ref[at : at + outer, :])
        two_ref[:outer, b * LANES : (b + 1) * LANES] = high
        two_ref[outer:, b * LANES : (b + 1) * LANES] = low
        at += outer

    def clear(g, carry):
        res[g] = jnp.zeros(res.shape[1:], jnp.float32)
        return carry

    lax.fori_loop(0, devices, clear, 0)

    def correlate(station):
        own_re, own_im = own[0], own[1]
        re = buf[station, :, 0].astype(jnp.float32).reshape(depth, column)
        im = buf[station, :, 1].astype(jnp.float32).reshape(depth, column)
        re_high, re_low = split(own_re * re + own_im * im)
        im_high, im_low = split(own_re * im - own_im * re)
        cross = jnp.concatenate([re_high, im_high, re_low, im_low, re_high, im_high], axis=0)
        mixed = jnp.dot(one_ref[...], cross, preferred_element_type=jnp.float32)
        real, imag = mixed[:inner], mixed[inner:]
        turned_re = real * twist_ref[0] - imag * twist_ref[1]
        turned_im = real * twist_ref[1] + imag * twist_ref[0]
        high, low = split(jnp.concatenate([turned_re, turned_im], axis=1))
        both = jnp.concatenate([high, low], axis=0)
        summed = lax.dot_general(
            two_ref[...],
            both,
            (((1,), (1,)), ((), ())),
            preferred_element_type=jnp.float32,
        )
        total = (summed[:outer, :inner] + summed[:outer, inner:]) + (
            summed[outer:, :inner] + summed[outer:, inner:]
        )
        flag = (mask_ref[0, station] * avail_ref[me] * avail_ref[station]).astype(jnp.float32)
        res[station] = total * (flag * scale)

    def column_in(p, k):
        arrived(index(p, side, core), p, k, 0)

        @pl.when(plane > 0)
        def _():
            down(p, k).start()

        if k < DETOUR:

            @pl.when((side == 0) | (p > plane + 1))
            def _():
                across(p, k).start()

        else:
            across(p, k).start()
        over(p, k).start()

    def side_in(p, k):
        arrived(index(p, 1 - side, core), p, k, 1)
        over_side(p, k).start()
        if k < DETOUR:

            @pl.when((p == plane) & (plane > 0))
            def _():
                down_side(k).start()

    def twin_column_in(p):
        for k in range(PIECES):
            arrived(index(p, side, 1 - core), p, k, 2)

    def twin_side_in(p):
        for k in range(PIECES):
            arrived(index(p, 1 - side, 1 - core), p, k, 3)

    @pl.when(core == 0)
    def _():
        twin_column_in(plane)
        correlate(twin)

    def step(p, carry):
        both = (side == 0) | (p > plane + 1)
        for k in range(PIECES):
            column_in(p, k)

            @pl.when(both)
            def _():
                side_in(p - 1, k)

        @pl.when(both)
        def _():
            correlate(index(p, side, core))
            correlate(index(p - 1, 1 - side, core))
            twin_column_in(p)
            twin_side_in(p - 1)
            correlate(index(p, side, 1 - core))
            correlate(index(p - 1, 1 - side, 1 - core))

        @pl.when(jnp.logical_not(both))
        def _():
            correlate(index(p, side, core))
            twin_column_in(p)
            correlate(index(p, side, 1 - core))

        return carry

    lax.fori_loop(plane + 1, planes, step, 0)

    @pl.when((side == 0) | (plane < planes - 1))
    def _():
        for k in range(PIECES):
            side_in(planes - 1, k)
        correlate(index(planes - 1, 1 - side, core))
        twin_side_in(planes - 1)
        correlate(index(planes - 1, 1 - side, 1 - core))

    group = math.gcd(devices, 8)

    def place(g, carry):
        at = pl.multiple_of(g * group, group)
        for o in range(outer):
            out_ref[pl.ds(at, group), o * inner : (o + 1) * inner] = res[pl.ds(at, group), o, :]
        return carry

    lax.fori_loop(0, devices // group, place, 0)

    for k in range(PIECES):

        @pl.when(plane > 0)
        def _():
            down(plane, k, True).wait_send()

        @pl.when(side == 1)
        def _():
            across(plane, k, True).wait_send()

        @pl.when(side == 0)
        def _():
            over_side(plane, k).wait_send()

        if k < DETOUR:

            @pl.when((side == 0) & (plane > 0))
            def _():
                down_side(k).wait_send()

        @pl.when(core == 1)
        def _():
            over(plane, k, True).wait_send()

    def finish(p, carry):
        for k in range(PIECES):

            @pl.when(plane > 0)
            def _():
                down(p, k).wait_send()

            if k < DETOUR:

                @pl.when((side == 0) | (p > plane + 1))
                def _():
                    across(p, k).wait_send()

            else:
                across(p, k).wait_send()
            over(p, k).wait_send()
            over_side(p, k).wait_send()
        return carry

    lax.fori_loop(plane + 1, planes, finish, 0)


def per_device(spectra, pair_mask, available):
    devices = lax.axis_size("row")
    freq = spectra.shape[2]
    packed, inner, column, outer = build_tables(freq, LAGS)
    depth = freq // column
    planes = devices // (LINE * CORES)
    shape = (PIECES, 2, depth // PIECES, column)
    vmem = pl.BlockSpec(memory_space=pltpu.VMEM)
    smem = pl.BlockSpec(memory_space=pltpu.SMEM)
    rows = pl.pallas_call(
        functools.partial(kernel, devices),
        out_shape=jax.ShapeDtypeStruct((devices, LAGS), jnp.float32),
        in_specs=[smem, smem, vmem, vmem],
        out_specs=vmem,
        scratch_shapes=[
            pltpu.VMEM((2 * inner, 3 * 2 * depth), jnp.bfloat16),
            pltpu.VMEM((2, inner, column), jnp.float32),
            pltpu.VMEM((2 * outer, 2 * column), jnp.bfloat16),
            pltpu.VMEM((devices, *shape), jnp.bfloat16),
            pltpu.VMEM((2, depth, column), jnp.float32),
            pltpu.VMEM((devices, outer, inner), jnp.float32),
            pltpu.SemaphoreType.DMA((4, planes, PIECES)),
            pltpu.SemaphoreType.DMA((planes, PIECES)),
            pltpu.SemaphoreType.DMA((planes, PIECES)),
            pltpu.SemaphoreType.DMA((2, planes, PIECES)),
        ],
        compiler_params=pltpu.CompilerParams(
            collective_id=0, has_side_effects=True, vmem_limit_bytes=48 * 1024 * 1024
        ),
    )(
        pair_mask,
        available,
        spectra.reshape(2, depth, column),
        jnp.asarray(packed),
    )
    return rows[None]


def solution(mesh):
    return jax.shard_map(
        per_device,
        mesh=mesh,
        in_specs=(P(("win", "row"), None, None), P("row", None), P("win")),
        out_specs=P(("win", "row"), None, None),
        check_vma=False,
    )
```

```python
import functools
import math

import jax
import jax.numpy as jnp
import numpy as np
from jax import lax
from jax.experimental import pallas as pl
from jax.experimental.pallas import tpu as pltpu
from jax.sharding import PartitionSpec as P

LAGS = 8192
MESH = pl.DeviceIdType.MESH
PIECES = 2
DETOUR = 1
LINE = 2
CORES = 2
LANES = 128


def split(value):
    high = value.astype(jnp.bfloat16)
    low = (value - high.astype(jnp.float32)).astype(jnp.bfloat16)
    return high, low


def build_tables(freq, lags):
    nfft = 2 * freq
    inner = min(128, lags // 2)
    column = nfft // inner
    depth = freq // column
    outer = lags // inner
    centre = lags // 2
    turn = 2.0 * np.pi
    t_inner = np.arange(inner)[:, None]
    first = turn * ((t_inner * np.arange(depth)[None, :]) % inner) / inner
    cos_first, sin_first = np.cos(first), np.sin(first)
    one = np.block([[cos_first, -sin_first], [sin_first, cos_first]]).astype(np.float32)
    k_column = np.arange(column)[None, :]
    twist = turn * ((k_column * (t_inner - centre)) % nfft) / nfft
    second = turn * ((np.arange(outer)[:, None] * k_column) % column) / column
    two = np.concatenate([np.cos(second), -np.sin(second)], axis=1).astype(np.float32)

    def stacked(table):
        return np.concatenate(np.split(table, table.shape[1] // LANES, axis=1), axis=0)

    turns = [np.cos(twist).astype(np.float32), np.sin(twist).astype(np.float32)]
    packed = np.concatenate([stacked(part) for part in (*turns, one, two)], axis=0)
    return packed, inner, column, outer


def kernel(
    devices,
    mask_ref,
    avail_ref,
    x_ref,
    packed_ref,
    out_ref,
    one_ref,
    twist_ref,
    two_ref,
    buf,
    own,
    res,
    recv,
    send_z,
    send_x,
    send_d,
    send_s,
):
    planes = devices // (LINE * CORES)
    me = lax.axis_index("row")
    core = me % CORES
    chip = me // CORES
    side = chip % LINE
    plane = chip // LINE
    depth, column = x_ref.shape[1:]
    rows = depth // PIECES
    inner = twist_ref.shape[1]
    outer = two_ref.shape[0] // 2
    scale = 2.0 / math.sqrt(8.0 * depth * column)

    def index(p, s, c):
        return (p * LINE + s) * CORES + c

    below = index(plane - 1, side, core)
    above = index(plane + 1, side, core)
    beside = index(plane, 1 - side, core)
    twin = index(plane, side, 1 - core)

    def greet(device):
        pl.semaphore_signal(barrier, inc=1, device_id={"row": device}, device_id_type=MESH)

    def copy(station, p, k, sem, kind, device, mine=False):
        slot = buf.at[station, k]
        return pltpu.make_async_remote_copy(
            src_ref=x_ref.at[:, pl.ds(k * rows, rows), :] if mine else slot,
            dst_ref=slot,
            send_sem=sem,
            recv_sem=recv.at[kind, p, k],
            device_id={"row": device},
            device_id_type=MESH,
        )

    def down(p, k, mine=False):
        return copy(index(p, side, core), p, k, send_z.at[p, k], 0, below, mine)

    def across(p, k, mine=False):
        return copy(index(p, side, core), p, k, send_x.at[p, k], 1, beside, mine)

    def over(p, k, mine=False):
        return copy(index(p, side, core), p, k, send_d.at[0, p, k], 2, twin, mine)

    def down_side(k):
        p = planes - 1
        return copy(index(p, 1 - side, core), p, k, send_s.at[k], 1, below)

    def over_side(p, k):
        return copy(index(p, 1 - side, core), p, k, send_d.at[1, p, k], 3, twin)

    def arrived(station, p, k, kind):
        slot = buf.at[station, k]
        pltpu.make_async_remote_copy(
            src_ref=slot,
            dst_ref=slot,
            send_sem=send_z.at[p, k],
            recv_sem=recv.at[kind, p, k],
            device_id={"row": twin},
            device_id_type=MESH,
        ).wait_recv()

    barrier = pltpu.get_barrier_semaphore()
    greet(beside)
    greet(twin)

    @pl.when(plane > 0)
    def _():
        greet(below)

    @pl.when(plane < planes - 1)
    def _():
        greet(above)

    peers = 2 + jnp.where(plane > 0, 1, 0) + jnp.where(plane < planes - 1, 1, 0)
    pl.semaphore_wait(barrier, peers)

    for k in range(PIECES):

        @pl.when(plane > 0)
        def _():
            down(plane, k, True).start()

        @pl.when(side == 1)
        def _():
            across(plane, k, True).start()

        @pl.when(core == 1)
        def _():
            over(plane, k, True).start()

    first = (
        (lax.broadcasted_iota(jnp.int32, (depth, column), 0) == 0)
        & (lax.broadcasted_iota(jnp.int32, (depth, column), 1) == 0)
    )
    weight = jnp.where(first, 0.5, 1.0)
    own[0] = x_ref[0].astype(jnp.float32) * weight
    own[1] = x_ref[1].astype(jnp.float32) * weight

    at = 0
    for part in range(2):
        for b in range(column // LANES):
            twist_ref[part, :, b * LANES : (b + 1) * LANES] = packed_ref[at : at + inner, :]
            at += inner
    for b in range(2 * depth // LANES):
        high, low = split(packed_ref[at : at + 2 * inner, :])
        for n, term in enumerate((high, high, low)):
            left = 2 * depth * n + b * LANES
            one_ref[:, left : left + LANES] = term
        at += 2 * inner
    for b in range(2 * column // LANES):
        high, low = split(packed_ref[at : at + outer, :])
        two_ref[:outer, b * LANES : (b + 1) * LANES] = high
        two_ref[outer:, b * LANES : (b + 1) * LANES] = low
        at += outer

    def clear(g, carry):
        res[g] = jnp.zeros(res.shape[1:], jnp.float32)
        return carry

    lax.fori_loop(0, devices, clear, 0)

    def correlate(station):
        own_re, own_im = own[0], own[1]
        re = buf[station, :, 0].astype(jnp.float32).reshape(depth, column)
        im = buf[station, :, 1].astype(jnp.float32).reshape(depth, column)
        re_high, re_low = split(own_re * re + own_im * im)
        im_high, im_low = split(own_re * im - own_im * re)
        cross = jnp.concatenate([re_high, im_high, re_low, im_low, re_high, im_high], axis=0)
        mixed = jnp.dot(one_ref[...], cross, preferred_element_type=jnp.float32)
        real, imag = mixed[:inner], mixed[inner:]
        turned_re = real * twist_ref[0] - imag * twist_ref[1]
        turned_im = real * twist_ref[1] + imag * twist_ref[0]
        high, low = split(jnp.concatenate([turned_re, turned_im], axis=1))
        both = jnp.concatenate([high, low], axis=0)
        summed = lax.dot_general(
            two_ref[...],
            both,
            (((1,), (1,)), ((), ())),
            preferred_element_type=jnp.float32,
        )
        total = (summed[:outer, :inner] + summed[:outer, inner:]) + (
            summed[outer:, :inner] + summed[outer:, inner:]
        )
        flag = (mask_ref[0, station] * avail_ref[me] * avail_ref[station]).astype(jnp.float32)
        res[station] = total * (flag * scale)

    def column_in(p, k):
        arrived(index(p, side, core), p, k, 0)

        @pl.when(plane > 0)
        def _():
            down(p, k).start()

        if k < DETOUR:

            @pl.when((side == 0) | (p < planes - 1))
            def _():
                across(p, k).start()

        else:
            across(p, k).start()
        over(p, k).start()

    def side_in(p, k):
        arrived(index(p, 1 - side, core), p, k, 1)
        over_side(p, k).start()
        if k < DETOUR:

            @pl.when((side == 0) & (plane > 0) & (p == planes - 1))
            def _():
                down_side(k).start()

    def twin_column_in(p):
        for k in range(PIECES):
            arrived(index(p, side, 1 - core), p, k, 2)

    def twin_side_in(p):
        for k in range(PIECES):
            arrived(index(p, 1 - side, 1 - core), p, k, 3)

    @pl.when(core == 0)
    def _():
        twin_column_in(plane)
        correlate(twin)

    def step(p, carry):
        both = (side == 0) | (p > plane + 1)
        for k in range(PIECES):
            column_in(p, k)

            @pl.when(both)
            def _():
                side_in(p - 1, k)

        @pl.when(both)
        def _():
            correlate(index(p, side, core))
            correlate(index(p - 1, 1 - side, core))
            twin_column_in(p)
            twin_side_in(p - 1)
            correlate(index(p, side, 1 - core))
            correlate(index(p - 1, 1 - side, 1 - core))

        @pl.when(jnp.logical_not(both))
        def _():
            correlate(index(p, side, core))
            twin_column_in(p)
            correlate(index(p, side, 1 - core))

        return carry

    lax.fori_loop(plane + 1, planes, step, 0)

    @pl.when((side == 0) | (plane < planes - 1))
    def _():
        for k in reversed(range(PIECES)):
            side_in(planes - 1, k)
        correlate(index(planes - 1, 1 - side, core))
        twin_side_in(planes - 1)
        correlate(index(planes - 1, 1 - side, 1 - core))

    group = math.gcd(devices, 8)

    def place(g, carry):
        at = pl.multiple_of(g * group, group)
        for o in range(outer):
            out_ref[pl.ds(at, group), o * inner : (o + 1) * inner] = res[pl.ds(at, group), o, :]
        return carry

    lax.fori_loop(0, devices // group, place, 0)

    for k in range(PIECES):

        @pl.when(plane > 0)
        def _():
            down(plane, k, True).wait_send()

        @pl.when(side == 1)
        def _():
            across(plane, k, True).wait_send()

        @pl.when(side == 0)
        def _():
            over_side(plane, k).wait_send()

        if k < DETOUR:

            @pl.when((side == 0) & (plane > 0))
            def _():
                down_side(k).wait_send()

        @pl.when(core == 1)
        def _():
            over(plane, k, True).wait_send()

    def finish(p, carry):
        for k in range(PIECES):

            @pl.when(plane > 0)
            def _():
                down(p, k).wait_send()

            if k < DETOUR:

                @pl.when((side == 0) | (p < planes - 1))
                def _():
                    across(p, k).wait_send()

            else:
                across(p, k).wait_send()
            over(p, k).wait_send()
            over_side(p, k).wait_send()
        return carry

    lax.fori_loop(plane + 1, planes, finish, 0)


def per_device(spectra, pair_mask, available):
    devices = lax.axis_size("row")
    freq = spectra.shape[2]
    packed, inner, column, outer = build_tables(freq, LAGS)
    depth = freq // column
    planes = devices // (LINE * CORES)
    shape = (PIECES, 2, depth // PIECES, column)
    vmem = pl.BlockSpec(memory_space=pltpu.VMEM)
    smem = pl.BlockSpec(memory_space=pltpu.SMEM)
    rows = pl.pallas_call(
        functools.partial(kernel, devices),
        out_shape=jax.ShapeDtypeStruct((devices, LAGS), jnp.float32),
        in_specs=[smem, smem, vmem, vmem],
        out_specs=vmem,
        scratch_shapes=[
            pltpu.VMEM((2 * inner, 3 * 2 * depth), jnp.bfloat16),
            pltpu.VMEM((2, inner, column), jnp.float32),
            pltpu.VMEM((2 * outer, 2 * column), jnp.bfloat16),
            pltpu.VMEM((devices, *shape), jnp.bfloat16),
            pltpu.VMEM((2, depth, column), jnp.float32),
            pltpu.VMEM((devices, outer, inner), jnp.float32),
            pltpu.SemaphoreType.DMA((4, planes, PIECES)),
            pltpu.SemaphoreType.DMA((planes, PIECES)),
            pltpu.SemaphoreType.DMA((planes, PIECES)),
            pltpu.SemaphoreType.DMA((2, planes, PIECES)),
            pltpu.SemaphoreType.DMA((DETOUR,)),
        ],
        compiler_params=pltpu.CompilerParams(
            collective_id=0, has_side_effects=True, vmem_limit_bytes=48 * 1024 * 1024
        ),
    )(
        pair_mask,
        available,
        spectra.reshape(2, depth, column),
        jnp.asarray(packed),
    )
    return rows[None]


def solution(mesh):
    return jax.shard_map(
        per_device,
        mesh=mesh,
        in_specs=(P(("win", "row"), None, None), P("row", None), P("win")),
        out_specs=P(("win", "row"), None, None),
        check_vma=False,
    )
```

```python
import functools
import math

import jax
import jax.numpy as jnp
import numpy as np
from jax import lax
from jax.experimental import pallas as pl
from jax.experimental.pallas import tpu as pltpu
from jax.sharding import PartitionSpec as P

LAGS = 8192
MESH = pl.DeviceIdType.MESH
PIECES = 2
DETOUR = 1
LINE = 2
CORES = 2
GRANT = 55_250_000
LANES = 128


def split(value):
    high = value.astype(jnp.bfloat16)
    low = (value - high.astype(jnp.float32)).astype(jnp.bfloat16)
    return high, low


def build_tables(freq, lags):
    nfft = 2 * freq
    inner = min(128, lags // 2)
    column = nfft // inner
    depth = freq // column
    outer = lags // inner
    centre = lags // 2
    turn = 2.0 * np.pi
    t_inner = np.arange(inner)[:, None]
    first = turn * ((t_inner * np.arange(depth)[None, :]) % inner) / inner
    cos_first, sin_first = np.cos(first), np.sin(first)
    one = np.block([[cos_first, -sin_first], [sin_first, cos_first]]).astype(np.float32)
    k_column = np.arange(column)[None, :]
    twist = turn * ((k_column * (t_inner - centre)) % nfft) / nfft
    second = turn * ((np.arange(outer)[:, None] * k_column) % column) / column
    two = np.concatenate([np.cos(second), -np.sin(second)], axis=1).astype(np.float32)

    def stacked(table):
        return np.concatenate(np.split(table, table.shape[1] // LANES, axis=1), axis=0)

    turns = [np.cos(twist).astype(np.float32), np.sin(twist).astype(np.float32)]
    packed = np.concatenate([stacked(part) for part in (*turns, one, two)], axis=0)
    return packed, inner, column, outer


def kernel(
    devices,
    mask_ref,
    avail_ref,
    x_ref,
    packed_hbm,
    out_ref,
    one_ref,
    twist_ref,
    two_ref,
    buf,
    own,
    res,
    recv,
    send_z,
    send_x,
    send_d,
    send_s,
    packed_ref,
    table_sem,
):
    planes = devices // (LINE * CORES)
    me = lax.axis_index("row")
    core = me % CORES
    chip = me // CORES
    side = chip % LINE
    plane = chip // LINE
    depth, column = x_ref.shape[1:]
    rows = depth // PIECES
    inner = twist_ref.shape[1]
    outer = two_ref.shape[0] // 2
    scale = 2.0 / math.sqrt(8.0 * depth * column)

    def index(p, s, c):
        return (p * LINE + s) * CORES + c

    below = index(plane - 1, side, core)
    above = index(plane + 1, side, core)
    beside = index(plane, 1 - side, core)
    twin = index(plane, side, 1 - core)

    def greet(device):
        pl.semaphore_signal(barrier, inc=1, device_id={"row": device}, device_id_type=MESH)

    def copy(station, p, k, sem, kind, device, mine=False):
        slot = buf.at[station, k]
        return pltpu.make_async_remote_copy(
            src_ref=x_ref.at[:, pl.ds(k * rows, rows), :] if mine else slot,
            dst_ref=slot,
            send_sem=sem,
            recv_sem=recv.at[kind, p, k],
            device_id={"row": device},
            device_id_type=MESH,
        )

    def down(p, k, mine=False):
        return copy(index(p, side, core), p, k, send_z.at[p, k], 0, below, mine)

    def across(p, k, mine=False):
        return copy(index(p, side, core), p, k, send_x.at[p, k], 1, beside, mine)

    def over(p, k, mine=False):
        return copy(index(p, side, core), p, k, send_d.at[0, p, k], 2, twin, mine)

    def down_side(k):
        p = planes - 1
        return copy(index(p, 1 - side, core), p, k, send_s.at[k], 1, below)

    def over_side(p, k):
        return copy(index(p, 1 - side, core), p, k, send_d.at[1, p, k], 3, twin)

    def arrived(station, p, k, kind):
        slot = buf.at[station, k]
        pltpu.make_async_remote_copy(
            src_ref=slot,
            dst_ref=slot,
            send_sem=send_z.at[p, k],
            recv_sem=recv.at[kind, p, k],
            device_id={"row": twin},
            device_id_type=MESH,
        ).wait_recv()

    load = pltpu.make_async_copy(packed_hbm, packed_ref, table_sem)
    load.start()
    barrier = pltpu.get_barrier_semaphore()
    greet(beside)
    greet(twin)

    @pl.when(plane > 0)
    def _():
        greet(below)

    @pl.when(plane < planes - 1)
    def _():
        greet(above)

    peers = 2 + jnp.where(plane > 0, 1, 0) + jnp.where(plane < planes - 1, 1, 0)
    pl.semaphore_wait(barrier, peers)

    for k in range(PIECES):

        @pl.when(plane > 0)
        def _():
            down(plane, k, True).start()

        @pl.when(side == 1)
        def _():
            across(plane, k, True).start()

        @pl.when(core == 1)
        def _():
            over(plane, k, True).start()

    first = (
        (lax.broadcasted_iota(jnp.int32, (depth, column), 0) == 0)
        & (lax.broadcasted_iota(jnp.int32, (depth, column), 1) == 0)
    )
    weight = jnp.where(first, 0.5, 1.0)
    own[0] = x_ref[0].astype(jnp.float32) * weight
    own[1] = x_ref[1].astype(jnp.float32) * weight

    load.wait()
    at = 0
    for part in range(2):
        for b in range(column // LANES):
            twist_ref[part, :, b * LANES : (b + 1) * LANES] = packed_ref[at : at + inner, :]
            at += inner
    for b in range(2 * depth // LANES):
        high, low = split(packed_ref[at : at + 2 * inner, :])
        for n, term in enumerate((high, high, low)):
            left = 2 * depth * n + b * LANES
            one_ref[:, left : left + LANES] = term
        at += 2 * inner
    for b in range(2 * column // LANES):
        high, low = split(packed_ref[at : at + outer, :])
        two_ref[:outer, b * LANES : (b + 1) * LANES] = high
        two_ref[outer:, b * LANES : (b + 1) * LANES] = low
        at += outer

    def clear(g, carry):
        res[g] = jnp.zeros(res.shape[1:], jnp.float32)
        return carry

    lax.fori_loop(0, devices, clear, 0)

    def correlate(station):
        own_re, own_im = own[0], own[1]
        re = buf[station, :, 0].astype(jnp.float32).reshape(depth, column)
        im = buf[station, :, 1].astype(jnp.float32).reshape(depth, column)
        re_high, re_low = split(own_re * re + own_im * im)
        im_high, im_low = split(own_re * im - own_im * re)
        cross = jnp.concatenate([re_high, im_high, re_low, im_low, re_high, im_high], axis=0)
        mixed = jnp.dot(one_ref[...], cross, preferred_element_type=jnp.float32)
        real, imag = mixed[:inner], mixed[inner:]
        turned_re = real * twist_ref[0] - imag * twist_ref[1]
        turned_im = real * twist_ref[1] + imag * twist_ref[0]
        high, low = split(jnp.concatenate([turned_re, turned_im], axis=1))
        both = jnp.concatenate([high, low], axis=0)
        summed = lax.dot_general(
            two_ref[...],
            both,
            (((1,), (1,)), ((), ())),
            preferred_element_type=jnp.float32,
        )
        total = (summed[:outer, :inner] + summed[:outer, inner:]) + (
            summed[outer:, :inner] + summed[outer:, inner:]
        )
        flag = (mask_ref[0, station] * avail_ref[me] * avail_ref[station]).astype(jnp.float32)
        res[station] = total * (flag * scale)

    def column_in(p, k):
        arrived(index(p, side, core), p, k, 0)

        @pl.when(plane > 0)
        def _():
            down(p, k).start()

        if k < DETOUR:

            @pl.when((side == 0) | (p < planes - 1))
            def _():
                across(p, k).start()

        else:
            across(p, k).start()
        over(p, k).start()

    def side_in(p, k):
        arrived(index(p, 1 - side, core), p, k, 1)
        over_side(p, k).start()
        if k < DETOUR:

            @pl.when((side == 0) & (plane > 0) & (p == planes - 1))
            def _():
                down_side(k).start()

    def twin_column_in(p):
        for k in range(PIECES):
            arrived(index(p, side, 1 - core), p, k, 2)

    def twin_side_in(p):
        for k in range(PIECES):
            arrived(index(p, 1 - side, 1 - core), p, k, 3)

    @pl.when(core == 0)
    def _():
        twin_column_in(plane)
        correlate(twin)

    def step(p, carry):
        both = (side == 0) | (p > plane + 1)
        for k in range(PIECES):
            column_in(p, k)

            @pl.when(both)
            def _():
                side_in(p - 1, k)

        @pl.when(both)
        def _():
            correlate(index(p, side, core))
            correlate(index(p - 1, 1 - side, core))
            twin_column_in(p)
            twin_side_in(p - 1)
            correlate(index(p, side, 1 - core))
            correlate(index(p - 1, 1 - side, 1 - core))

        @pl.when(jnp.logical_not(both))
        def _():
            correlate(index(p, side, core))
            twin_column_in(p)
            correlate(index(p, side, 1 - core))

        return carry

    lax.fori_loop(plane + 1, planes, step, 0)

    @pl.when((side == 0) | (plane < planes - 1))
    def _():
        for k in reversed(range(PIECES)):
            side_in(planes - 1, k)
        correlate(index(planes - 1, 1 - side, core))
        twin_side_in(planes - 1)
        correlate(index(planes - 1, 1 - side, 1 - core))

    group = math.gcd(devices, 8)

    def place(g, carry):
        at = pl.multiple_of(g * group, group)
        for o in range(outer):
            out_ref[pl.ds(at, group), o * inner : (o + 1) * inner] = res[pl.ds(at, group), o, :]
        return carry

    lax.fori_loop(0, devices // group, place, 0)

    for k in range(PIECES):

        @pl.when(plane > 0)
        def _():
            down(plane, k, True).wait_send()

        @pl.when(side == 1)
        def _():
            across(plane, k, True).wait_send()

        @pl.when(side == 0)
        def _():
            over_side(plane, k).wait_send()

        if k < DETOUR:

            @pl.when((side == 0) & (plane > 0))
            def _():
                down_side(k).wait_send()

        @pl.when(core == 1)
        def _():
            over(plane, k, True).wait_send()

    def finish(p, carry):
        for k in range(PIECES):

            @pl.when(plane > 0)
            def _():
                down(p, k).wait_send()

            if k < DETOUR:

                @pl.when((side == 0) | (p < planes - 1))
                def _():
                    across(p, k).wait_send()

            else:
                across(p, k).wait_send()
            over(p, k).wait_send()
            over_side(p, k).wait_send()
        return carry

    lax.fori_loop(plane + 1, planes, finish, 0)


def per_device(spectra, pair_mask, available):
    devices = lax.axis_size("row")
    freq = spectra.shape[2]
    packed, inner, column, outer = build_tables(freq, LAGS)
    depth = freq // column
    planes = devices // (LINE * CORES)
    shape = (PIECES, 2, depth // PIECES, column)
    vmem = pl.BlockSpec(memory_space=pltpu.VMEM)
    smem = pl.BlockSpec(memory_space=pltpu.SMEM)
    rows = pl.pallas_call(
        functools.partial(kernel, devices),
        out_shape=jax.ShapeDtypeStruct((devices, LAGS), jnp.float32),
        in_specs=[smem, smem, vmem, pl.BlockSpec(memory_space=pltpu.HBM)],
        out_specs=vmem,
        scratch_shapes=[
            pltpu.VMEM((2 * inner, 3 * 2 * depth), jnp.bfloat16),
            pltpu.VMEM((2, inner, column), jnp.float32),
            pltpu.VMEM((2 * outer, 2 * column), jnp.bfloat16),
            pltpu.VMEM((devices, *shape), jnp.bfloat16),
            pltpu.VMEM((2, depth, column), jnp.float32),
            pltpu.VMEM((devices, outer, inner), jnp.float32),
            pltpu.SemaphoreType.DMA((4, planes, PIECES)),
            pltpu.SemaphoreType.DMA((planes, PIECES)),
            pltpu.SemaphoreType.DMA((planes, PIECES)),
            pltpu.SemaphoreType.DMA((2, planes, PIECES)),
            pltpu.SemaphoreType.DMA((DETOUR,)),
            pltpu.VMEM(packed.shape, jnp.float32),
            pltpu.SemaphoreType.DMA(()),
        ],
        compiler_params=pltpu.CompilerParams(
            collective_id=0, has_side_effects=True, vmem_limit_bytes=GRANT
        ),
    )(
        pair_mask,
        available,
        spectra.reshape(2, depth, column),
        jnp.asarray(packed),
    )
    return rows[None]


def solution(mesh):
    return jax.shard_map(
        per_device,
        mesh=mesh,
        in_specs=(P(("win", "row"), None, None), P("row", None), P("win")),
        out_specs=P(("win", "row"), None, None),
        check_vma=False,
    )
```
